32 devices in a mesh: fac: 8 (over z, y), cust: 4 (over x, core).
Axes of the slice: x: 2, y: 2, z: 4, core: 2. Of those that a mesh axis runs over, the one named last changes fastest.
Arguments:
- fac_coords: bfloat16 [4096, 128], P('fac'), may hold values from -6 to 6
- cust_coords: bfloat16 [65536, 128], P(('cust', 'fac')), may hold values from -6 to 6
- open_flags: int32 [4096], P('fac'), may hold values 0 or 1
- demand: int32 [65536], P('cust'), may hold values from 1 to 4
- fixed_cost: float32 [4096], P('fac'), may hold values from 0 to 64
- capacity: float32 [4096], P('fac'), may hold values from 32 to 128
- cap_mult: float32 [4096], P('fac'), may hold values from 0 to 0.1
- cover_mult: float32 [65536], P('cust'), may hold values from 0 to 2, as said below
Outputs:
- cover_final: float32 [65536], P('cust')
- cap_final: float32 [4096], P('fac')
- bounds: float32 [3], replicated
The draws below stay inside these ranges and needn't reach their ends.
Inputs may be any that keep to these rules, and one draw needn't show every extreme that they name: `cover_mult`: initial coverage multipliers, all in one band of width 0.4.
All inputs are finite; a program needn't handle non-finite values. No bound on the sum of `open_flags` on one device may be relied on, other than what follows from the above.
Results may differ from the reference program's by a relative error of at most 0.0003.
Values may be sent and summed in bfloat16 or wider, within the bound.
A program may use at most 64 MiB of HBM per device.

```python
import math
import jax
import jax.numpy as jnp
from jax import lax

K = 128
ITERS = 3
F = 4096
C = 65536


def draw_cover_mult(key, part):
    tau = 0.1
    level = 2.125 - tau * (math.log(F / 2.0) + 300.0 / K)
    spread = jax.random.uniform(key, (C,), jnp.float32, -0.2, 0.2)
    return (level + spread).astype(jnp.float32)


def with_ends(array, rng, smallest, top_value):
    index_at = [jax.random.randint(jax.random.fold_in(rng, axis), (), 0, length) for axis, length in enumerate(array.shape)]
    longest = array.shape.index(max(array.shape))
    neighbour = index_at[:longest] + [(index_at[longest] + 1) % array.shape[longest]] + index_at[longest + 1:]
    return array.at[tuple(index_at)].set(smallest).at[tuple(neighbour)].set(top_value)


def levels(own_key, dims, split, low, high):
    def one(dim, blocks):
        heights = jax.random.uniform(jax.random.fold_in(jax.random.fold_in(own_key, 6), dim), (blocks,), jnp.float32, low / len(split), high / len(split))
        return jnp.repeat(jnp.exp(heights), dims[dim] // blocks).reshape((-1,) + (1,) * (len(dims) - dim - 1))

    loudness = one(*split[0])
    for cut in split[1:]:
        loudness = loudness * one(*cut)
    return loudness


def noise(stream_key, shape, scale, reach, pieces=(), kind=jnp.bfloat16):
    gain = levels(stream_key, shape, pieces, -0.22, 0.18) if pieces else 1.0
    entries = jax.random.normal(stream_key, shape, jnp.float32) * scale * gain
    return jnp.minimum(jnp.maximum(entries, -reach), reach).astype(kind)


def setup_inputs(seed: int = 0) -> dict:
    key_of = jax.random.split(jax.random.key(seed), 9)
    return {
        "fac_coords": noise(key_of[0], (F, K), 1.0, 6.0, ((0, 8),)),
        "cust_coords": noise(key_of[1], (C, K), 1.0, 6.0, ((0, 32),)),
        "open_flags": with_ends((jax.random.randint(key_of[2], (F,), 0, 2) < 1).astype(jnp.int32), jax.random.fold_in(key_of[2], 1), 0, 1),
        "demand": with_ends(jax.random.randint(key_of[3], (C,), 1, 5), jax.random.fold_in(key_of[3], 1), 1, 4).astype(jnp.int32),
        "fixed_cost": jnp.clip(64.0 * jax.random.uniform(key_of[4], (F,), jnp.float32) ** levels(key_of[4], (F,), ((0, 8),), -0.2, 0.2), 0.0, 64.0),
        "capacity": jnp.clip(32.0 + 96.0 * jax.random.uniform(key_of[5], (F,), jnp.float32) ** levels(key_of[5], (F,), ((0, 8),), -0.2, 0.2), 32.0, 128.0),
        "cap_mult": jnp.clip(0.1 * jax.random.uniform(key_of[6], (F,), jnp.float32) ** levels(key_of[6], (F,), ((0, 8),), -0.2, 0.2), 0.0, 0.1),
        "cover_mult": draw_cover_mult(jax.random.fold_in(key_of[8], 71), 0),
    }


def reference(fac_coords, cust_coords, open_flags, demand, fixed_cost, capacity, cap_mult, cover_mult):
    tau = 0.1
    fac_block = 256
    n_fac = fac_coords.shape[0]
    n_cust = cust_coords.shape[0]
    width = fac_coords.shape[1]
    fac_block = min(fac_block, n_fac)
    opened = open_flags.astype(jnp.float32)
    weight = demand.astype(jnp.float32)
    pnorm = jnp.sum(fac_coords.astype(jnp.float32) ** 2, axis=1)
    qnorm = jnp.sum(cust_coords.astype(jnp.float32) ** 2, axis=1)
    blocks = n_fac // fac_block
    lam = cover_mult
    mu = cap_mult
    bound_list = []
    for step in range(ITERS):
        size = 0.1 / (step + 1)

        def one_block(cover, index):
            start = (index * fac_block).astype(jnp.int32)
            rows = lax.dynamic_slice_in_dim(fac_coords, start, fac_block, 0)
            pn = lax.dynamic_slice_in_dim(pnorm, start, fac_block, 0)
            mu_b = lax.dynamic_slice_in_dim(mu, start, fac_block, 0)
            op_b = lax.dynamic_slice_in_dim(opened, start, fac_block, 0)
            dots = lax.dot_general(rows, cust_coords, (((1,), (1,)), ((), ())), preferred_element_type=jnp.float32)
            cost = (pn[:, None] + qnorm[None, :] - 2.0 * dots) / width
            zval = (lam[None, :] - cost - mu_b[:, None] * weight[None, :]) / tau
            share = op_b[:, None] * jax.nn.sigmoid(zval)
            load_b = jnp.sum(share * weight[None, :], axis=1)
            soft_b = -tau * op_b * jnp.sum(jax.nn.softplus(zval) * weight[None, :], axis=1)
            return cover + jnp.sum(share, axis=0), (load_b, soft_b)

        cover, pair = lax.scan(one_block, jnp.zeros((n_cust,), jnp.float32), jnp.arange(blocks, dtype=jnp.int32))
        load = pair[0].reshape(n_fac)
        soft = pair[1].reshape(n_fac)
        bound = (jnp.sum(weight * lam) + jnp.sum(opened * fixed_cost - mu * capacity + soft)) / n_cust
        bound_list.append(bound)
        lam = lam + size * weight * (1.0 - cover) / (1.0 + cover)
        mu = jnp.maximum(0.0, mu + size * (load - capacity) / (load + capacity))
    return lam, mu, jnp.stack(bound_list).astype(jnp.float32)
```

```python
import functools
import math

import jax
import jax.numpy as jnp
from jax import lax
from jax.experimental import pallas as pl
from jax.experimental.pallas import tpu as pltpu
from jax.sharding import PartitionSpec as P

MESH = pl.DeviceIdType.MESH
ITERS = 3
TAU = 0.1
LAG = 3
CLOSED = -30000.0
F32 = jnp.float32
BF16 = jnp.bfloat16
VMEM = pl.BlockSpec(memory_space=pltpu.VMEM)


def split3(v):
    a = v.astype(BF16)
    r = v - a.astype(F32)
    b = r.astype(BF16)
    c = (r - b.astype(F32)).astype(BF16)
    return a, b, c


def nt(a, b):
    return lax.dot_general(a, b, (((1,), (1,)), ((), ())), preferred_element_type=F32)


def eye_of(rows, width):
    hit = lax.broadcasted_iota(jnp.int32, (rows, width), 0) == lax.broadcasted_iota(jnp.int32, (rows, width), 1)
    return hit.astype(F32).astype(BF16)


def onehot_of(open_row, rows):
    n = open_row.shape[1]
    flags = jnp.broadcast_to(open_row.astype(F32), (16, n)).astype(BF16)
    tri = (lax.broadcasted_iota(jnp.int32, (n, n), 0) <= lax.broadcasted_iota(jnp.int32, (n, n), 1)).astype(F32).astype(BF16)
    pos = jnp.dot(flags, tri, preferred_element_type=F32)[0:1]
    pos = jnp.where(open_row > 0, pos - 1.0, -1.0).astype(jnp.int32)
    hit = lax.broadcasted_iota(jnp.int32, (rows, n), 0) == pos
    return jnp.where(hit, 1.0, 0.0).astype(BF16)


def solve_kernel(nf, nc, rows, total_cust,
                 open_ref, fac_ref, cap_ref, mu_in_ref, fixed_ref, cust_ref, demand_ref, cover_ref,
                 lam_out, cap_out, bound_out, flag_out,
                 facs, infos, hot_ref, side, w_ref, y_ref, acc, cov_ref, soft_ref, d_ref, hq_ref, lam_ref, mus, caps,
                 tot_ref, pay, got1, mid, got2,
                 s1, r1, s2, r2, s3, r3, s4, r4, s5, r5, s6, r6):
    f, c = lax.axis_index("fac"), lax.axis_index("cust")
    n, width = fac_ref.shape
    cols = cust_ref.shape[0]
    part = infos.shape[3]
    padded = part * nc
    wide = pay.shape[2]
    half = nc // 2
    core = lax.rem(c, 2)
    twin = (f, c + 1 - 2 * core)
    barrier = pltpu.get_barrier_semaphore()
    for d in range(1, nf):
        pl.semaphore_signal(barrier, inc=1, device_id=(lax.rem(f + d, nf), c), device_id_type=MESH)
    for d in range(1, nc):
        pl.semaphore_signal(barrier, inc=1, device_id=(f, lax.rem(c + d, nc)), device_id_type=MESH)

    opened = open_ref[...].astype(F32)
    hot = onehot_of(open_ref[...], padded)
    hot_ref[...] = hot
    fac = fac_ref[...]
    facs[f] = jnp.dot(hot, fac, preferred_element_type=F32).astype(BF16)
    q1, q2, _ = split3(fac.astype(F32) ** 2)
    ones = jnp.ones((16, width), BF16)
    halfsq = -0.5 * (nt(ones, q1) + nt(ones, q2))[0:1]
    rows16 = [jnp.ones((1, n), BF16)]
    for v in (halfsq, mu_in_ref[...], cap_ref[...]):
        rows16.extend(split3(v))
    rows16 = [r.astype(F32) for r in rows16] + [jnp.zeros((6, n), F32)]
    got = nt(jnp.concatenate(rows16, axis=0).astype(BF16), hot)
    bias = jnp.where(got[0:1] > 0, got[1:2] + got[2:3] + got[3:4], CLOSED)
    count = jnp.broadcast_to(jnp.sum(opened, axis=1, keepdims=True), (1, padded))
    info = jnp.concatenate([bias, got[4:5] + got[5:6] + got[6:7], got[7:8] + got[8:9] + got[9:10], count, jnp.zeros((4, padded), F32)], axis=0)
    for p in range(nc):
        infos[f, p] = info[:, p * part:(p + 1) * part]

    def rows_of(q):
        return pl.ds(pl.multiple_of(q * part, 16), part)

    def move(src, q, send, recv, peer):
        a, b = facs.at[src, rows_of(q)], infos.at[src, q]
        return [pltpu.make_async_remote_copy(a, a, send.at[0], recv.at[0], device_id=peer, device_id_type=MESH),
                pltpu.make_async_remote_copy(b, b, send.at[1], recv.at[1], device_id=peer, device_id_type=MESH)]

    def first_copy(src, dst, peer_f):
        return move(src, c, s1.at[dst], r1.at[src], (peer_f, c))

    def side_copy(src, e, q):
        return move(src, q, s2.at[src, e], r2.at[src, e], (f, lax.rem(c + 2 * (e + 1), nc)))

    def twin_copy(src, e, q):
        return move(src, q, s3.at[src, e], r3.at[src, e], twin)

    pl.semaphore_wait(barrier, nf + nc - 2)
    for d in sorted(range(1, nf), key=lambda v: abs(v - nf // 2)):
        peer = lax.rem(f + d, nf)
        for cpy in first_copy(f, peer, peer):
            cpy.start()

    ext = jnp.zeros((1, 128), F32)
    lane = lax.broadcasted_iota(jnp.int32, (1, 128), 1)
    shut = mu_in_ref[...]
    for k in range(ITERS):
        fixed = jnp.sum(opened * fixed_ref[...] - (1.0 - opened) * shut * cap_ref[...])
        ext = ext + jnp.where((lane == k) & (c == 0), fixed, 0.0)
        shut = jnp.maximum(0.0, shut - 0.1 / (k + 1))
    tot_ref[...] = ext
    mine = pl.ds(pl.multiple_of(f * cols, cols), cols)
    wt = demand_ref[:, mine].astype(F32)
    lam = cover_ref[:, mine]
    lam_ref[...] = lam
    d_ref[...] = jnp.broadcast_to(wt, (8, cols))
    turned = nt(eye_of(width, width), cust_ref[...])
    w_ref[0:width, :] = turned.astype(BF16)
    hq = 0.5 * jnp.sum(turned * turned, axis=0, keepdims=True)
    hq_ref[...] = hq
    w_ref[width:, :] = jnp.zeros((width, cols), BF16)
    sel = eye_of(16, width)
    acc[...] = jnp.zeros_like(acc)
    pay[...] = jnp.zeros_like(pay)

    def set_aug(lam):
        a1, a2, a3 = split3(64.0 * lam - hq_ref[...])
        aug = jnp.concatenate([a1.astype(F32), a2.astype(F32), a3.astype(F32), jnp.ones((3, cols), F32),
                               jnp.broadcast_to(-64.0 * d_ref[0:1, :], (3, cols)), jnp.zeros((7, cols), F32)], axis=0)
        w_ref[width:width + 16, :] = aug.astype(BF16)

    def forward_first(b):
        @pl.when(b != f)
        def _():
            for cpy in first_copy(b, f, f):
                cpy.wait_recv()
            for e in range(half - 1):
                for cpy in side_copy(b, e, c):
                    cpy.start()
            for cpy in twin_copy(b, 0, c):
                cpy.start()

    def forward_side(b):
        @pl.when(b != f)
        def _():
            for e in range(half - 1):
                q = lax.rem(c + nc - 2 * (e + 1), nc)
                for cpy in side_copy(b, e, q):
                    cpy.wait_recv()
                for cpy in twin_copy(b, e + 1, q):
                    cpy.start()

    def arrived(b):
        @pl.when(b != f)
        def _():
            for e in range(half):
                for cpy in twin_copy(b, e, rows_from(e)):
                    cpy.wait_recv()

    def rows_from(e):
        return lax.rem(twin[1] + nc - 2 * e, nc)

    def prepare(b, k):
        if k == 0:
            inf = jnp.concatenate([infos[b, p] for p in range(nc)], axis=1)
            mu, cap = inf[1:2], inf[2:3]
            caps[b] = inf
            bias = inf[0:1]
        else:
            g = (k - 1) * nf + b
            wait_second(g)
            inf = caps[b]
            bias, cap = inf[0:1], inf[2:3]
            load = total_of(g)[:, 0:padded]
            mu = mus[b]
            mu = jnp.maximum(0.0, mu + (0.1 / k) * (load - cap) / (load + jnp.where(cap > 0, cap, 1.0)))
        mus[b] = mu
        parts = [p.astype(F32) for p in split3(bias) + split3(mu)]
        stack = jnp.concatenate([jnp.ones((3, padded), F32)] + parts + [jnp.zeros((7, padded), F32)], axis=0).astype(BF16)
        col = lax.dot_general(stack, sel, (((0,), (0,)), ((), ())), preferred_element_type=F32).astype(BF16)
        side[b] = col

    def first_sum(g, e, peer):
        return pltpu.make_async_remote_copy(pay.at[g], got1.at[g, e], s4.at[g], r4.at[g], device_id=peer, device_id_type=MESH)

    def second_sum(g, d, peer):
        return pltpu.make_async_remote_copy(mid.at[g], got2.at[g, d], s5.at[g], r5.at[g], device_id=peer, device_id_type=MESH)

    def all_first(g):
        return pltpu.make_async_remote_copy(got1.at[g], got1.at[g], s4.at[g], r4.at[g], device_id=twin, device_id_type=MESH)

    def all_second(g):
        return pltpu.make_async_remote_copy(got2.at[g], got2.at[g], s5.at[g], r5.at[g], device_id=twin, device_id_type=MESH)

    def wait_second(g):
        all_second(g).wait_recv()

    def total_of(g):
        total = mid[g]
        for d in range(nf - 1):
            total = total + got2[g, d]
        return total

    def pass_on(g):
        all_first(g).wait_recv()
        total = pay[g]
        for e in range(nc - 1):
            total = total + got1[g, e]
        mid[g] = total
        for d in range(1, nf):
            second_sum(g, d - 1, (lax.rem(f + d, nf), c)).start()

    block = y_ref.shape[2]
    tiles = cols // block
    groups = block // 128
    scale = math.log2(math.e) / 6.4

    def dot(b, t, slot):
        lhs = jnp.concatenate([facs[b, 0:rows], side[b, 0:rows]], axis=1)
        y_ref[slot] = jnp.dot(lhs, w_ref[:, t * block:(t + 1) * block], preferred_element_type=F32)

    def tile(t, slot):
        at = [slice(t * block + q * 128, t * block + (q + 1) * 128) for q in range(groups)]
        covs = [cov_ref[:, a] for a in at]
        softs = [soft_ref[:, a] for a in at]
        ds = [d_ref[:, a] for a in at]
        for r in range(0, rows, 32):
            size = min(4, (rows - r) // 8)
            sums = [None] * size
            for q in range(groups):
                es = [jnp.exp2(y_ref[slot, r + 8 * s:r + 8 * s + 8, q * 128:(q + 1) * 128] * scale) for s in range(size)]
                us = [1.0 + e for e in es]
                p01 = us[0] * us[1]
                if size == 4:
                    p23 = us[2] * us[3]
                    p = p01 * p23
                    inv = ds[q] * (1.0 / p)
                    r01, r23 = inv * p23, inv * p01
                    xs = [es[0] * (us[1] * r01), es[1] * (us[0] * r01), es[2] * (us[3] * r23), es[3] * (us[2] * r23)]
                    covs[q] = covs[q] + ((xs[0] + xs[1]) + (xs[2] + xs[3]))
                else:
                    p = p01
                    inv = ds[q] * (1.0 / p)
                    xs = [es[0] * (us[1] * inv), es[1] * (us[0] * inv)]
                    covs[q] = covs[q] + (xs[0] + xs[1])
                softs[q] = softs[q] + jnp.log(p)
                sums = [x if s is None else s + x for s, x in zip(sums, xs)]
            for s in range(size):
                lo = r + 8 * s
                acc[lo:lo + 8, :] = sums[s] if t == 0 else acc[lo:lo + 8, :] + sums[s]
        for q in range(groups):
            cov_ref[:, at[q]] = covs[q]
            soft_ref[:, at[q]] = softs[q]

    set_aug(lam)
    if nf > 1:
        forward_first(0)
        forward_first(1)
        forward_side(0)
        arrived(0)
    ones16 = jnp.ones((16, 128), BF16)

    for k in range(ITERS):
        cov_ref[...] = jnp.zeros_like(cov_ref)
        soft_ref[...] = jnp.zeros_like(soft_ref)
        if k == 0:
            forward_first(2)
            forward_side(1)
        prepare(0, k)
        dot(0, 0, 0)

        def body(b, _, k=k):
            g = k * nf + b
            nxt = lax.rem(b + 1, nf)
            for t in range(tiles - 1):
                dot(b, t + 1, (t + 1) % 2)
                tile(t, t % 2)

            @pl.when(b + 1 < nf)
            def _():
                if k == 0:
                    @pl.when(b + 3 < nf)
                    def _():
                        forward_first(b + 3)

                    @pl.when(b + 2 < nf)
                    def _():
                        forward_side(b + 2)
                    arrived(b + 1)
                prepare(b + 1, k)
            dot(nxt, 0, tiles % 2)
            tile(tiles - 1, (tiles - 1) % 2)
            part_sum = acc[...]
            hi = part_sum.astype(BF16)
            lo = (part_sum - hi.astype(F32)).astype(BF16)
            row = (nt(ones16, hi) + nt(ones16, lo))[0:1]
            pay[g, :, 0:padded] = row
            if k == ITERS - 1:
                @pl.when(b == nf - 1)
                def _():
                    finish_step(k)
            for e in range(nc - 1):
                first_sum(g, e, (f, lax.rem(c + e + 1, nc))).start()

            if k == 0:
                @pl.when(b >= LAG)
                def _():
                    pass_on(g - LAG)
            else:
                pass_on(g - LAG)
            return 0

        def finish_step(k):
            wt = d_ref[0:1, :]
            lam = lam_ref[...]
            cover = jnp.sum(cov_ref[...], axis=0, keepdims=True) / wt
            soft = jnp.sum(soft_ref[...], axis=0, keepdims=True)
            held = jnp.sum(mus[f] * caps[f, 2:3])
            here = jnp.sum(wt * lam - TAU * wt * soft) - jnp.where(c == 0, held, 0.0)
            tot = tot_ref[...] + jnp.where(lane == k, here, 0.0)
            tot_ref[...] = tot
            lam = lam + (0.1 / (k + 1)) * wt * (1.0 - cover) / (1.0 + cover)
            lam_ref[...] = lam
            if k == ITERS - 1:
                pay[ITERS * nf - 1, :, wide - 128:] = tot
            else:
                set_aug(lam)

        lax.fori_loop(0, nf, body, 0)
        if k < ITERS - 1:
            finish_step(k)

    def lam_copy(src, dst, peer_f):
        return pltpu.make_async_remote_copy(lam_ref, lam_out.at[src], s6.at[dst], r6.at[src], device_id=(peer_f, c), device_id_type=MESH)

    for d in range(1, nf):
        peer = lax.rem(f + d, nf)
        lam_copy(f, peer, peer).start()
    lam_out[f] = lam_ref[...]
    last = ITERS * nf

    def flush(i, _):
        pass_on(last - LAG + i)
        return 0

    lax.fori_loop(0, min(LAG, nf), flush, 0)

    def drain(i, _):
        wait_second(last - nf + i)
        return 0

    lax.fori_loop(0, nf, drain, 0)
    load = total_of(last - nf + f)[:, 0:padded]
    inf = caps[f]
    cap = inf[2:3]
    mu = mus[f]
    mu = jnp.maximum(0.0, mu + (0.1 / ITERS) * (load - cap) / (load + jnp.where(cap > 0, cap, 1.0)))
    stack = jnp.concatenate([v.astype(F32) for v in split3(mu)] + [jnp.zeros((13, padded), F32)], axis=0).astype(BF16)
    back = jnp.dot(stack, hot_ref[...], preferred_element_type=F32)
    shut = mu_in_ref[...]
    for k in range(ITERS):
        shut = jnp.maximum(0.0, shut - 0.1 / (k + 1))
    cap_out[...] = jnp.where(open_ref[...] > 0, back[0:1] + back[1:2] + back[2:3], shut)
    bound_out[...] = total_of(last - 1)[:, wide - 128:] / total_cust
    most = jnp.max(jnp.max(caps[:, 3, :], axis=0, keepdims=True), axis=1, keepdims=True)
    flag_out[...] = jnp.broadcast_to((most > rows).astype(jnp.int32), (1, 128))

    def close(j, _):
        src = lax.rem(f + j, nf)
        for cpy in first_copy(f, src, src):
            cpy.wait_send()
        lam_copy(src, src, src).wait()
        for e in range(half - 1):
            for cpy in side_copy(src, e, c):
                cpy.wait_send()
        for e in range(half):
            for cpy in twin_copy(src, e, c):
                cpy.wait_send()
        return 0

    lax.fori_loop(1, nf, close, 0)

    def settle(g, _):
        all_first(g).wait_send()
        all_second(g).wait_send()
        return 0

    lax.fori_loop(0, last, settle, 0)


def local(nf, nc, fac_coords, cust_coords, open_flags, demand, fixed_cost, capacity, cap_mult, cover_mult):
    n, width = fac_coords.shape
    cols = cust_coords.shape[0]
    sd = jax.ShapeDtypeStruct
    dma = pltpu.SemaphoreType.DMA
    half = nc // 2
    open_row = open_flags.reshape(1, n)
    block = math.gcd(cols, 512) if cols > 512 else cols // 2
    args = (open_row, fac_coords, capacity.reshape(1, n), cap_mult.reshape(1, n), fixed_cost.reshape(1, n), cust_coords,
            demand.reshape(1, nf * cols), cover_mult.reshape(1, nf * cols))

    def run(rows, cid):
        part = -(-rows // (16 * nc)) * 16
        padded = part * nc
        wide = -(-padded // 128) * 128 + 128
        last = ITERS * nf
        return pl.pallas_call(
            functools.partial(solve_kernel, nf, nc, rows, cols * nf * nc),
            out_shape=(sd((nf, 1, cols), F32), sd((1, n), F32), sd((1, 128), F32), sd((1, 128), jnp.int32)),
            in_specs=[VMEM] * 8, out_specs=(VMEM,) * 4,
            scratch_shapes=[
                pltpu.VMEM((nf, padded, width), BF16),
                pltpu.VMEM((nf, nc, 8, part), F32),
                pltpu.VMEM((padded, n), BF16),
                pltpu.VMEM((nf, padded, width), BF16),
                pltpu.VMEM((2 * width, cols), BF16),
                pltpu.VMEM((2, rows, block), F32),
                pltpu.VMEM((padded, 128), F32),
                pltpu.VMEM((8, cols), F32),
                pltpu.VMEM((8, cols), F32),
                pltpu.VMEM((8, cols), F32),
                pltpu.VMEM((1, cols), F32),
                pltpu.VMEM((1, cols), F32),
                pltpu.VMEM((nf, 1, padded), F32),
                pltpu.VMEM((nf, 8, padded), F32),
                pltpu.VMEM((1, 128), F32),
                pltpu.VMEM((last, 1, wide), F32),
                pltpu.VMEM((last, nc - 1, 1, wide), F32),
                pltpu.VMEM((last, 1, wide), F32),
                pltpu.VMEM((last, nf - 1, 1, wide), F32),
                dma((nf, 2)), dma((nf, 2)),
                dma((nf, half - 1, 2)), dma((nf, half - 1, 2)),
                dma((nf, half, 2)), dma((nf, half, 2)),
                dma((last,)), dma((last,)), dma((last,)), dma((last,)),
                dma((nf,)), dma((nf,)),
            ],
            compiler_params=pltpu.CompilerParams(collective_id=cid, has_side_effects=True, vmem_limit_bytes=56 * 2 ** 20),
            name="solve",
        )(*args)

    rows = min(n, -(-int(n / 2 + 2 * math.sqrt(n)) // 16) * 16)
    lam, cap, bound, flag = run(rows, 0)
    if rows < n:
        lam, cap, bound = lax.cond(flag[0, 0] > 0, lambda: tuple(run(n, 1)[:3]), lambda: (lam, cap, bound))
    return lam.reshape(nf * cols), cap.reshape(n), bound[0, :ITERS]


def solution(mesh):
    nf, nc = mesh.shape["fac"], mesh.shape["cust"]
    return jax.shard_map(
        functools.partial(local, nf, nc),
        mesh=mesh,
        in_specs=(P("fac", None), P(("cust", "fac"), None), P("fac"), P("cust"), P("fac"), P("fac"), P("fac"), P("cust")),
        out_specs=(P("cust"), P("fac"), P()),
        check_vma=False,
    )
```

```python
import functools
import math

import jax
import jax.numpy as jnp
from jax import lax
from jax.experimental import pallas as pl
from jax.experimental.pallas import tpu as pltpu
from jax.sharding import PartitionSpec as P

MESH = pl.DeviceIdType.MESH
ITERS = 3
TAU = 0.1
LAG = 3
CLOSED = -30000.0
F32 = jnp.float32
BF16 = jnp.bfloat16
VMEM = pl.BlockSpec(memory_space=pltpu.VMEM)
SMEM = pl.BlockSpec(memory_space=pltpu.SMEM)
HBM = pl.BlockSpec(memory_space=pltpu.HBM)


def split3(v):
    a = v.astype(BF16)
    r = v - a.astype(F32)
    b = r.astype(BF16)
    c = (r - b.astype(F32)).astype(BF16)
    return a, b, c


def nt(a, b):
    return lax.dot_general(a, b, (((1,), (1,)), ((), ())), preferred_element_type=F32)


def eye_of(rows, width):
    hit = lax.broadcasted_iota(jnp.int32, (rows, width), 0) == lax.broadcasted_iota(jnp.int32, (rows, width), 1)
    return hit.astype(F32).astype(BF16)


def onehot_of(open_row, rows):
    n = open_row.shape[1]
    flags = jnp.broadcast_to(open_row.astype(F32), (16, n)).astype(BF16)
    tri = (lax.broadcasted_iota(jnp.int32, (n, n), 0) <= lax.broadcasted_iota(jnp.int32, (n, n), 1)).astype(F32).astype(BF16)
    pos = jnp.dot(flags, tri, preferred_element_type=F32)[0:1]
    pos = jnp.where(open_row > 0, pos - 1.0, -1.0).astype(jnp.int32)
    hit = lax.broadcasted_iota(jnp.int32, (rows, n), 0) == pos
    return jnp.where(hit, 1.0, 0.0).astype(BF16)


def solve_kernel(nf, nc, rows, total_cust,
                 open_in, fac_in, cap_in, mu_in, fixed_in, cust_in, demand_in, cover_in,
                 lam_out, cap_out, bound_out, flag_out,
                 open_ref, fac_ref, cap_ref, mu_in_ref, fixed_ref, cust_ref, demand_ref, cover_ref, loads,
                 facs, infos, hot_ref, side, w_ref, y_ref, acc, cov_ref, soft_ref, d_ref, hq_ref, lam_ref, mus, caps,
                 tot_ref, dl_ref, pay, got1, mid, got2,
                 s1, r1, s2, r2, s3, r3, s4, r4, s5, r5, s6, r6):
    f, c = lax.axis_index("fac"), lax.axis_index("cust")
    n, width = fac_ref.shape
    cols = cust_ref.shape[0]
    part = infos.shape[3]
    padded = part * nc
    wide = pay.shape[2]
    half = nc // 2
    core = lax.rem(c, 2)
    twin = (f, c + 1 - 2 * core)
    barrier = pltpu.get_barrier_semaphore()
    for d in range(1, nf):
        pl.semaphore_signal(barrier, inc=1, device_id=(lax.rem(f + d, nf), c), device_id_type=MESH)
    for d in range(1, nc):
        pl.semaphore_signal(barrier, inc=1, device_id=(f, lax.rem(c + d, nc)), device_id_type=MESH)

    mine = pl.ds(pl.multiple_of(f * cols, cols), cols)
    fetch = [pltpu.make_async_copy(src, dst, loads.at[i]) for i, (src, dst) in enumerate([
        (open_in, open_ref), (fac_in, fac_ref), (cap_in, cap_ref), (mu_in, mu_in_ref),
        (fixed_in, fixed_ref), (cust_in, cust_ref), (demand_in.at[:, mine], demand_ref), (cover_in.at[:, mine], cover_ref)])]
    for cpy in fetch:
        cpy.start()
    for cpy in fetch[:4]:
        cpy.wait()

    opened = open_ref[...].astype(F32)
    hot = onehot_of(open_ref[...], padded)
    hot_ref[...] = hot
    fac = fac_ref[...]
    facs[f] = jnp.dot(hot, fac, preferred_element_type=F32).astype(BF16)
    q1, q2, _ = split3(fac.astype(F32) ** 2)
    ones = jnp.ones((16, width), BF16)
    halfsq = -0.5 * (nt(ones, q1) + nt(ones, q2))[0:1]
    rows16 = [jnp.ones((1, n), BF16)]
    for v in (halfsq, mu_in_ref[...], cap_ref[...]):
        rows16.extend(split3(v))
    rows16 = [r.astype(F32) for r in rows16] + [jnp.zeros((6, n), F32)]
    got = nt(jnp.concatenate(rows16, axis=0).astype(BF16), hot)
    bias = jnp.where(got[0:1] > 0, got[1:2] + got[2:3] + got[3:4], CLOSED)
    count = jnp.broadcast_to(jnp.sum(opened, axis=1, keepdims=True), (1, padded))
    info = jnp.concatenate([bias, got[4:5] + got[5:6] + got[6:7], got[7:8] + got[8:9] + got[9:10], count], axis=0)
    for p in range(nc):
        infos[f, p] = info[:, p * part:(p + 1) * part]

    def rows_of(q):
        return pl.ds(pl.multiple_of(q * part, 16), part)

    def bulk(ref, send, recv):
        return pltpu.make_async_remote_copy(ref, ref, send, recv, device_id=twin, device_id_type=MESH)

    def move(src, q, send, recv, peer):
        a, b = facs.at[src, rows_of(q)], infos.at[src, q]
        return [pltpu.make_async_remote_copy(a, a, send.at[0], recv.at[0], device_id=peer, device_id_type=MESH),
                pltpu.make_async_remote_copy(b, b, send.at[1], recv.at[1], device_id=peer, device_id_type=MESH)]

    def first_copy(src, peer_f):
        return move(src, c, s1, r1.at[src], (peer_f, c))

    def side_copy(src, e, q):
        return move(src, q, s2, r2.at[src, e], (f, lax.rem(c + 2 * (e + 1), nc)))

    def twin_copy(src, q):
        return move(src, q, s3, r3.at[src], twin)

    pl.semaphore_wait(barrier, nf + nc - 2)
    upper = f // (nf // 2)
    for j in range(nf - 1):
        down = nf - 2 - j + (nf - 2 - j + nf - f) // nf
        up = j + (j + nf - f) // nf
        for cpy in first_copy(f, upper * up + (1 - upper) * down):
            cpy.start()

    for cpy in fetch[4:]:
        cpy.wait()
    ext = jnp.zeros((1, 128), F32)
    lane = lax.broadcasted_iota(jnp.int32, (1, 128), 1)
    shut = mu_in_ref[...]
    for k in range(ITERS):
        fixed = jnp.sum(opened * fixed_ref[...] - (1.0 - opened) * shut * cap_ref[...])
        ext = ext + jnp.where((lane == k) & (c == 0), fixed, 0.0)
        shut = jnp.maximum(0.0, shut - 0.1 / (k + 1))
    tot_ref[...] = ext
    wt = demand_ref[...].astype(F32)
    lam = cover_ref[...]
    lam_ref[...] = lam
    d_ref[...] = jnp.broadcast_to(wt, (8, cols))
    turned = nt(eye_of(width, width), cust_ref[...])
    w_ref[0:width, :] = turned.astype(BF16)
    hq = 0.5 * jnp.sum(turned * turned, axis=0, keepdims=True)
    hq_ref[...] = hq
    w_ref[width:, :] = jnp.zeros((width, cols), BF16)
    sel = eye_of(16, width)
    acc[...] = jnp.zeros_like(acc)
    lanes_d = jnp.zeros((1, 128), F32)
    for t in range(cols // 128):
        lanes_d = lanes_d + wt[:, t * 128:(t + 1) * 128]
    dl_ref[...] = lanes_d
    pay[...] = jnp.zeros_like(pay)

    def set_aug(lam):
        a1, a2, a3 = split3(64.0 * lam - hq_ref[...])
        aug = jnp.concatenate([a1.astype(F32), a2.astype(F32), a3.astype(F32), jnp.ones((3, cols), F32),
                               jnp.broadcast_to(-64.0 * d_ref[0:1, :], (3, cols)), jnp.zeros((7, cols), F32)], axis=0)
        w_ref[width:width + 16, :] = aug.astype(BF16)

    def forward_first(b):
        @pl.when(b != f)
        def _():
            for cpy in first_copy(b, f):
                cpy.wait_recv()
            for e in range(half - 1):
                for cpy in side_copy(b, e, c):
                    cpy.start()
            for cpy in twin_copy(b, c):
                cpy.start()

    def forward_side(b):
        @pl.when(b != f)
        def _():
            for e in range(half - 1):
                q = lax.rem(c + nc - 2 * (e + 1), nc)
                for cpy in side_copy(b, e, q):
                    cpy.wait_recv()
                for cpy in twin_copy(b, q):
                    cpy.start()

    def arrived(b):
        @pl.when(b != f)
        def _():
            bulk(facs.at[b, 0:half * part], s3.at[0], r3.at[b, 0]).wait_recv()
            bulk(infos.at[b, 0:half], s3.at[1], r3.at[b, 1]).wait_recv()

    def prepare(b, k):
        if k == 0:
            inf = jnp.concatenate([infos[b, p] for p in range(nc)], axis=1)
            bias, mu = inf[0:1], inf[1:2]
            caps[b] = inf
        else:
            g = (k - 1) * nf + b
            inf = caps[b]
            bias, cap = inf[0:1], inf[2:3]
            load = total_of(g)[:, 0:padded]
            mu = jnp.maximum(0.0, mus[g] + (0.1 / k) * (load - cap) / (load + jnp.where(cap > 0, cap, 1.0)))
        mus[k * nf + b] = mu
        parts = [p.astype(F32) for p in split3(bias) + split3(mu)]
        stack = jnp.concatenate([jnp.ones((3, padded), F32)] + parts + [jnp.zeros((7, padded), F32)], axis=0).astype(BF16)
        side[b] = lax.dot_general(stack, sel, (((0,), (0,)), ((), ())), preferred_element_type=F32).astype(BF16)

    def first_sum(g, e, peer):
        return pltpu.make_async_remote_copy(pay.at[g], got1.at[g, e], s4, r4.at[g], device_id=peer, device_id_type=MESH)

    def second_sum(g, d, peer):
        return pltpu.make_async_remote_copy(mid.at[g], got2.at[g, d], s5, r5.at[g], device_id=peer, device_id_type=MESH)

    def wait_second(g):
        bulk(got2.at[g], s5, r5.at[g]).wait_recv()

    def total_of(g):
        total = mid[g]
        for d in range(nf - 1):
            total = total + got2[g, d]
        return total

    def pass_on(g):
        bulk(got1.at[g], s4, r4.at[g]).wait_recv()
        total = pay[g]
        for e in range(nc - 1):
            total = total + got1[g, e]
        mid[g] = total
        for d in range(1, nf):
            second_sum(g, d - 1, (lax.rem(f + d, nf), c)).start()

    block = y_ref.shape[2]
    tiles = cols // block
    groups = block // 128
    scale = math.log2(math.e) / 6.4

    def dot(b, t, slot):
        lhs = jnp.concatenate([facs[b, 0:rows], side[b, 0:rows]], axis=1)
        y_ref[slot] = jnp.dot(lhs, w_ref[:, t * block:(t + 1) * block], preferred_element_type=F32)

    def tile(b, t, slot):
        at = [slice(t * block + q * 128, t * block + (q + 1) * 128) for q in range(groups)]
        covs = [cov_ref[:, a] for a in at]
        softs = [soft_ref[:, a] for a in at]
        ds = [d_ref[:, a] for a in at]
        for r in range(0, rows, 32):
            size = min(4, (rows - r) // 8)
            sums = [None] * size
            for q in range(groups):
                us = [1.0 + jnp.exp2(y_ref[slot, r + 8 * s:r + 8 * s + 8, q * 128:(q + 1) * 128] * scale) for s in range(size)]
                gs = []
                p = None
                for s in range(0, size, 2):
                    pair = us[s] * us[s + 1]
                    inv = ds[q] * (1.0 / pair)
                    gs += [us[s + 1] * inv, us[s] * inv]
                    p = pair if p is None else p * pair
                held = gs[0] + gs[1]
                if size == 4:
                    held = held + (gs[2] + gs[3])
                covs[q] = covs[q] + (float(size) * ds[q] - held)
                softs[q] = softs[q] + jnp.log2(p)
                sums = [g if v is None else v + g for v, g in zip(sums, gs)]
            for s in range(size):
                lo = r + 8 * s
                acc[b, lo:lo + 8, :] = sums[s] if t == 0 else acc[b, lo:lo + 8, :] + sums[s]
        for q in range(groups):
            cov_ref[:, at[q]] = covs[q]
            soft_ref[:, at[q]] = softs[q]

    ones16 = jnp.ones((16, 128), BF16)
    live = lax.broadcasted_iota(jnp.int32, (padded, 128), 0) < rows

    def row_of(b, g):
        part_sum = jnp.where(live, dl_ref[...] - acc[b], 0.0)
        hi = part_sum.astype(BF16)
        lo = (part_sum - hi.astype(F32)).astype(BF16)
        pay[g, :, 0:padded] = (nt(ones16, hi) + nt(ones16, lo))[0:1]

    def send_row(g):
        for e in range(nc - 1):
            first_sum(g, e, (f, lax.rem(c + e + 1, nc))).start()

    pair = f - lax.rem(f, 2)

    def place(k, p):
        if k > 0:
            return p
        q = p - 2
        far = q + 2 * ((q + nf - pair) // nf)
        return jnp.where(p == 0, f, jnp.where(p == 1, 2 * pair + 1 - f, far))

    def finish_step(k):
        wt = d_ref[0:1, :]
        lam = lam_ref[...]
        cover = jnp.sum(cov_ref[...], axis=0, keepdims=True) / wt
        soft = math.log(2.0) * jnp.sum(soft_ref[...], axis=0, keepdims=True)
        held = jnp.sum(mus[k * nf + f] * caps[f, 2:3])
        here = jnp.sum(wt * lam - TAU * wt * soft) - jnp.where(c == 0, held, 0.0)
        tot = tot_ref[...] + jnp.where(lane == k, here, 0.0)
        tot_ref[...] = tot
        lam = lam + (0.1 / (k + 1)) * wt * (1.0 - cover) / (1.0 + cover)
        lam_ref[...] = lam
        if k == ITERS - 1:
            pay[ITERS * nf - 1, :, wide - 128:] = tot
        else:
            set_aug(lam)

    def gather_turn(p):
        for i in range(3):
            at = 3 * p - 1 + i

            @pl.when((at > 0) & (at < nf))
            def _():
                forward_first(place(0, at))

        @pl.when(p < 2)
        def _():
            forward_side(place(0, p + 1))

        @pl.when((p > 0) & (p + 2 < nf))
        def _():
            forward_side(place(0, p + 2))

        @pl.when(p + 1 < nf)
        def _():
            arrived(place(0, p + 1))

    set_aug(lam)
    for k in range(ITERS):
        cov_ref[...] = jnp.zeros_like(cov_ref)
        soft_ref[...] = jnp.zeros_like(soft_ref)
        start = f if k == 0 else 0
        if k > 0:
            wait_second((k - 1) * nf)
        prepare(start, k)
        dot(start, 0, 0)

        def body(p, _, k=k):
            b = place(k, p)
            nxt = place(k, lax.rem(p + 1, nf))
            if k == 0:
                before = place(0, lax.rem(p + nf - 1, nf))
            elif k == 1:
                before = jnp.where(p == 0, place(0, nf - 1), nf + p - 1)
            else:
                before = k * nf + p - 1
            if k == 0:
                row_of(before, before)
            else:
                row_of(lax.rem(before, nf), before)
            for t in range(tiles // 2):
                dot(b, t + 1, (t + 1) % 2)
                tile(b, t, t % 2)
            if k == 0:
                @pl.when(p > 0)
                def _():
                    send_row(before)

                @pl.when(p >= LAG)
                def _():
                    pass_on(place(0, p - LAG))
                gather_turn(p)
            else:
                send_row(before)
                if k == 1:
                    pass_on(jnp.where(p < LAG, place(0, nf + p - LAG), nf + p - LAG))
                else:
                    pass_on(k * nf + p - LAG)

                @pl.when(p + 1 < nf)
                def _():
                    wait_second((k - 1) * nf + p + 1)
            for t in range(tiles // 2, tiles - 1):
                dot(b, t + 1, (t + 1) % 2)
                tile(b, t, t % 2)
            prepare(nxt, k)
            dot(nxt, 0, tiles % 2)
            tile(b, tiles - 1, (tiles - 1) % 2)
            return 0

        lax.fori_loop(0, nf, body, 0)
        finish_step(k)

    last = ITERS * nf
    row_of(nf - 1, last - 1)
    send_row(last - 1)

    for d in range(1, nf):
        pltpu.make_async_remote_copy(lam_ref, lam_out.at[f], s6, r6, device_id=(lax.rem(f + d, nf), c), device_id_type=MESH).start()
    lam_out[f] = lam_ref[...]
    for send, recv, width_parts in ((s1, r1, 1), (s2, r2, half - 1), (s3, r3, half)):
        bulk(facs.at[0:nf - 1, 0:width_parts * part], send.at[0], recv.at[(0,) * (len(recv.shape) - 1) + (0,)]).wait_send()
        bulk(infos.at[0:nf - 1, 0:width_parts], send.at[1], recv.at[(0,) * (len(recv.shape) - 1) + (1,)]).wait_send()

    def flush(i, _):
        pass_on(last - LAG + i)
        return 0

    lax.fori_loop(0, LAG, flush, 0)

    def drain(i, _):
        wait_second(last - nf + i)
        return 0

    lax.fori_loop(0, nf, drain, 0)
    load = total_of(last - nf + f)[:, 0:padded]
    inf = caps[f]
    cap = inf[2:3]
    mu = mus[last - nf + f]
    mu = jnp.maximum(0.0, mu + (0.1 / ITERS) * (load - cap) / (load + jnp.where(cap > 0, cap, 1.0)))
    stack = jnp.concatenate([v.astype(F32) for v in split3(mu)] + [jnp.zeros((13, padded), F32)], axis=0).astype(BF16)
    back = jnp.dot(stack, hot_ref[...], preferred_element_type=F32)
    shut = mu_in_ref[...]
    for k in range(ITERS):
        shut = jnp.maximum(0.0, shut - 0.1 / (k + 1))
    cap_out[...] = jnp.where(open_ref[...] > 0, back[0:1] + back[1:2] + back[2:3], shut)
    bound_out[...] = total_of(last - 1)[:, wide - 128:] / total_cust
    most = jnp.max(jnp.max(caps[:, 3, :], axis=0, keepdims=True), axis=1, keepdims=True)
    flag_out[0, 0] = (most[0, 0] > rows).astype(jnp.int32)

    lams = bulk(lam_out.at[0:nf - 1], s6, r6)
    lams.wait_send()
    lams.wait_recv()
    bulk(got1, s4, r4.at[0]).wait_send()
    bulk(got2, s5, r5.at[0]).wait_send()


def finish_kernel(lam_ref, cap_ref, bound_ref, lam_out, cap_out, bound_out):
    lam_out[...] = lam_ref[...]
    cap_out[...] = cap_ref[...]
    bound_out[...] = bound_ref[:, 0:bound_out.shape[1]]


def local(nf, nc, fac_coords, cust_coords, open_flags, demand, fixed_cost, capacity, cap_mult, cover_mult):
    n, width = fac_coords.shape
    cols = cust_coords.shape[0]
    sd = jax.ShapeDtypeStruct
    dma = pltpu.SemaphoreType.DMA
    half = nc // 2
    open_row = open_flags.reshape(1, n)
    block = math.gcd(cols, 256)
    args = (open_row, fac_coords, capacity.reshape(1, n), cap_mult.reshape(1, n), fixed_cost.reshape(1, n), cust_coords,
            demand.reshape(1, nf * cols), cover_mult.reshape(1, nf * cols))

    def run(rows, cid):
        part = -(-rows // (16 * nc)) * 16
        padded = part * nc
        wide = -(-padded // 128) * 128 + 128
        last = ITERS * nf
        return pl.pallas_call(
            functools.partial(solve_kernel, nf, nc, rows, cols * nf * nc),
            out_shape=(sd((nf, 1, cols), F32), sd((1, n), F32), sd((1, 128), F32), sd((1, 1), jnp.int32)),
            in_specs=[HBM] * 8, out_specs=(VMEM,) * 3 + (SMEM,),
            scratch_shapes=[
                pltpu.VMEM((1, n), jnp.int32),
                pltpu.VMEM((n, width), BF16),
                pltpu.VMEM((1, n), F32),
                pltpu.VMEM((1, n), F32),
                pltpu.VMEM((1, n), F32),
                pltpu.VMEM((cols, width), BF16),
                pltpu.VMEM((1, cols), jnp.int32),
                pltpu.VMEM((1, cols), F32),
                dma((8,)),
                pltpu.VMEM((nf, padded, width), BF16),
                pltpu.VMEM((nf, nc, 4, part), F32),
                pltpu.VMEM((padded, n), BF16),
                pltpu.VMEM((nf, padded, width), BF16),
                pltpu.VMEM((2 * width, cols), BF16),
                pltpu.VMEM((2, rows, block), F32),
                pltpu.VMEM((nf, padded, 128), F32),
                pltpu.VMEM((8, cols), F32),
                pltpu.VMEM((8, cols), F32),
                pltpu.VMEM((8, cols), F32),
                pltpu.VMEM((1, cols), F32),
                pltpu.VMEM((1, cols), F32),
                pltpu.VMEM((last, 1, padded), F32),
                pltpu.VMEM((nf, 4, padded), F32),
                pltpu.VMEM((1, 128), F32),
                pltpu.VMEM((1, 128), F32),
                pltpu.VMEM((last, 1, wide), F32),
                pltpu.VMEM((last, nc - 1, 1, wide), F32),
                pltpu.VMEM((last, 1, wide), F32),
                pltpu.VMEM((last, nf - 1, 1, wide), F32),
                dma((2,)), dma((nf, 2)),
                dma((2,)), dma((nf, half - 1, 2)),
                dma((2,)), dma((nf, 2)),
                dma(()), dma((last,)), dma(()), dma((last,)),
                dma(()), dma(()),
            ],
            compiler_params=pltpu.CompilerParams(collective_id=cid, has_side_effects=True, vmem_limit_bytes=56 * 2 ** 20),
            name="solve",
        )(*args)

    rows = min(n, -(-int(n / 2 + 2 * math.sqrt(n)) // 16) * 16)
    lam, cap, bound, flag = run(rows, 0)
    if rows < n:
        lam, cap, bound = lax.cond(flag[0, 0] > 0, lambda: tuple(run(n, 1)[:3]), lambda: (lam, cap, bound))
    lam, cap, bound = pl.pallas_call(
        finish_kernel, out_shape=(sd((nf, 1, cols), F32), sd((1, n), F32), sd((1, ITERS), F32)),
        in_specs=[VMEM] * 3, out_specs=(VMEM,) * 3, name="finish",
    )(lam, cap, bound)
    return lam.reshape(nf * cols), cap.reshape(n), bound.reshape(ITERS)


def solution(mesh):
    nf, nc = mesh.shape["fac"], mesh.shape["cust"]
    return jax.shard_map(
        functools.partial(local, nf, nc),
        mesh=mesh,
        in_specs=(P("fac", None), P(("cust", "fac"), None), P("fac"), P("cust"), P("fac"), P("fac"), P("fac"), P("cust")),
        out_specs=(P("cust"), P("fac"), P()),
        check_vma=False,
    )
```

```python
import functools
import math

import jax
import jax.numpy as jnp
from jax import lax
from jax.experimental import pallas as pl
from jax.experimental.pallas import tpu as pltpu
from jax.sharding import PartitionSpec as P

MESH = pl.DeviceIdType.MESH
ITERS = 3
TAU = 0.1
LAG = 3
CLOSED = -30000.0
F32 = jnp.float32
BF16 = jnp.bfloat16
VMEM = pl.BlockSpec(memory_space=pltpu.VMEM)
SMEM = pl.BlockSpec(memory_space=pltpu.SMEM)
HBM = pl.BlockSpec(memory_space=pltpu.HBM)


def split3(v):
    a = v.astype(BF16)
    r = v - a.astype(F32)
    b = r.astype(BF16)
    c = (r - b.astype(F32)).astype(BF16)
    return a, b, c


def nt(a, b):
    return lax.dot_general(a, b, (((1,), (1,)), ((), ())), preferred_element_type=F32)


def eye_of(rows, width):
    hit = lax.broadcasted_iota(jnp.int32, (rows, width), 0) == lax.broadcasted_iota(jnp.int32, (rows, width), 1)
    return hit.astype(F32).astype(BF16)


def onehot_of(open_row, rows):
    n = open_row.shape[1]
    flags = jnp.broadcast_to(open_row.astype(F32), (16, n)).astype(BF16)
    tri = (lax.broadcasted_iota(jnp.int32, (n, n), 0) <= lax.broadcasted_iota(jnp.int32, (n, n), 1)).astype(F32).astype(BF16)
    pos = jnp.dot(flags, tri, preferred_element_type=F32)[0:1]
    pos = jnp.where(open_row > 0, pos - 1.0, -1.0).astype(jnp.int32)
    hit = lax.broadcasted_iota(jnp.int32, (rows, n), 0) == pos
    return jnp.where(hit, 1.0, 0.0).astype(BF16)


def solve_kernel(nf, nc, rows, total_cust,
                 first, *refs):
    small_in, (fac_in, cust_in, demand_in, cover_in), refs = (refs[:4], refs[4:8], refs[8:]) if first else (refs[0], refs[1:5], refs[5:])
    (lam_out, cap_out, bound_out), refs = refs[:3], refs[3:]
    if first:
        (flag_out, small_out), refs = refs[:2], refs[2:]
    (open_ref, fac_ref, cap_ref, mu_in_ref, fixed_ref, cust_ref, demand_ref, cover_ref, loads,
                 facs, infos, hot_ref, side, w_ref, y_ref, acc, cov_ref, soft_ref, d_ref, hq_ref, lam_ref, mus, caps,
                 tot_ref, dl_ref, pay, got1, mid, got2,
                 s1, r1, s2, r2, s3, r3, s4, r4, s5, r5, s6, r6) = refs
    f, c = lax.axis_index("fac"), lax.axis_index("cust")
    n, width = fac_ref.shape
    cols = cust_ref.shape[0]
    part = infos.shape[3]
    padded = part * nc
    wide = pay.shape[2]
    half = nc // 2
    core = lax.rem(c, 2)
    twin = (f, c + 1 - 2 * core)
    barrier = pltpu.get_barrier_semaphore()
    for d in range(1, nf):
        pl.semaphore_signal(barrier, inc=1, device_id=(lax.rem(f + d, nf), c), device_id_type=MESH)
        pl.semaphore_signal(barrier, inc=1, device_id=(lax.rem(f + d, nf), twin[1]), device_id_type=MESH)
    for d in range(1, nc):
        pl.semaphore_signal(barrier, inc=1, device_id=(f, lax.rem(c + d, nc)), device_id_type=MESH)

    mine = pl.ds(pl.multiple_of(f * cols, cols), cols)
    pairs = [(fac_in, fac_ref), (cust_in, cust_ref), (demand_in.at[:, mine], demand_ref), (cover_in.at[:, mine], cover_ref)]
    if first:
        pairs += list(zip(small_in, (open_ref, cap_ref, mu_in_ref, fixed_ref)))
    fetch = [pltpu.make_async_copy(src, dst, loads.at[i]) for i, (src, dst) in enumerate(pairs)]
    for cpy in fetch:
        cpy.start()
    for cpy in fetch[:1] + fetch[4:]:
        cpy.wait()
    if first:
        small_out[0:1, :] = open_ref[...].astype(F32)
        for i, ref in enumerate((cap_ref, mu_in_ref, fixed_ref)):
            small_out[i + 1:i + 2, :] = ref[...]
    else:
        open_ref[...] = small_in[0:1, :].astype(jnp.int32)
        for i, ref in enumerate((cap_ref, mu_in_ref, fixed_ref)):
            ref[...] = small_in[i + 1:i + 2, :]

    opened = open_ref[...].astype(F32)
    hot = onehot_of(open_ref[...], padded)
    hot_ref[...] = hot
    fac = fac_ref[...]
    facs[f] = jnp.dot(hot, fac, preferred_element_type=F32).astype(BF16)
    q1, q2, _ = split3(fac.astype(F32) ** 2)
    ones = jnp.ones((16, width), BF16)
    halfsq = -0.5 * (nt(ones, q1) + nt(ones, q2))[0:1]
    rows16 = [jnp.ones((1, n), BF16)]
    for v in (halfsq, mu_in_ref[...], cap_ref[...]):
        rows16.extend(split3(v))
    rows16 = [r.astype(F32) for r in rows16] + [jnp.zeros((6, n), F32)]
    got = nt(jnp.concatenate(rows16, axis=0).astype(BF16), hot)
    bias = jnp.where(got[0:1] > 0, got[1:2] + got[2:3] + got[3:4], CLOSED)
    count = jnp.broadcast_to(jnp.sum(opened, axis=1, keepdims=True), (1, padded))
    info = jnp.concatenate([bias, got[4:5] + got[5:6] + got[6:7], got[7:8] + got[8:9] + got[9:10], count], axis=0)
    for p in range(nc):
        infos[f, p] = info[:, p * part:(p + 1) * part]

    def rows_of(q):
        return pl.ds(pl.multiple_of(q * part, 16), part)

    def bulk(ref, send, recv):
        return pltpu.make_async_remote_copy(ref, ref, send, recv, device_id=twin, device_id_type=MESH)

    def move(src, q, send, recv, peer):
        a, b = facs.at[src, rows_of(q)], infos.at[src, q]
        return [pltpu.make_async_remote_copy(a, a, send.at[0], recv.at[0], device_id=peer, device_id_type=MESH),
                pltpu.make_async_remote_copy(b, b, send.at[1], recv.at[1], device_id=peer, device_id_type=MESH)]

    def first_copy(src, peer_f, peer_c):
        return move(src, peer_c, s1, r1.at[src], (peer_f, peer_c))

    def side_copy(src, e, q):
        return move(src, q, s2, r2.at[src, e], (f, lax.rem(c + 2 * (e + 1), nc)))

    def twin_copy(src, q):
        return move(src, q, s3, r3.at[src], twin)

    pl.semaphore_wait(barrier, 2 * (nf - 1) + nc - 1)
    upper = f // (nf // 2)

    @pl.when(core == 1)
    def _():
        for j in range(nf - 1):
            down = nf - 2 - j + (nf - 2 - j + nf - f) // nf
            up = j + (j + nf - f) // nf
            for peer_c in (c - 1, c):
                for cpy in first_copy(f, upper * up + (1 - upper) * down, peer_c):
                    cpy.start()

    for cpy in fetch[1:4]:
        cpy.wait()
    ext = jnp.zeros((1, 128), F32)
    lane = lax.broadcasted_iota(jnp.int32, (1, 128), 1)
    shut = mu_in_ref[...]
    for k in range(ITERS):
        fixed = jnp.sum(opened * fixed_ref[...] - (1.0 - opened) * shut * cap_ref[...])
        ext = ext + jnp.where((lane == k) & (c == 0), fixed, 0.0)
        shut = jnp.maximum(0.0, shut - 0.1 / (k + 1))
    tot_ref[...] = ext
    wt = demand_ref[...].astype(F32)
    lam = cover_ref[...]
    lam_ref[...] = lam
    d_ref[...] = jnp.broadcast_to(wt, (8, cols))
    turned = nt(eye_of(width, width), cust_ref[...])
    w_ref[0:width, :] = turned.astype(BF16)
    hq = 0.5 * jnp.sum(turned * turned, axis=0, keepdims=True)
    hq_ref[...] = hq
    w_ref[width:, :] = jnp.zeros((width, cols), BF16)
    sel = eye_of(16, width)
    acc[...] = jnp.zeros_like(acc)
    lanes_d = jnp.zeros((1, 128), F32)
    for t in range(cols // 128):
        lanes_d = lanes_d + wt[:, t * 128:(t + 1) * 128]
    dl_ref[...] = lanes_d
    pay[...] = jnp.zeros_like(pay)

    def set_aug(lam):
        a1, a2, a3 = split3(64.0 * lam - hq_ref[...])
        aug = jnp.concatenate([a1.astype(F32), a2.astype(F32), a3.astype(F32), jnp.ones((3, cols), F32),
                               jnp.broadcast_to(-64.0 * d_ref[0:1, :], (3, cols)), jnp.zeros((7, cols), F32)], axis=0)
        w_ref[width:width + 16, :] = aug.astype(BF16)

    def forward_first(b):
        @pl.when(b != f)
        def _():
            for cpy in first_copy(b, f, c):
                cpy.wait_recv()
            for e in range(half - 1):
                for cpy in side_copy(b, e, c):
                    cpy.start()
            for cpy in twin_copy(b, c):
                cpy.start()

    def forward_side(b):
        @pl.when(b != f)
        def _():
            for e in range(half - 1):
                q = lax.rem(c + nc - 2 * (e + 1), nc)
                for cpy in side_copy(b, e, q):
                    cpy.wait_recv()
                for cpy in twin_copy(b, q):
                    cpy.start()

    def arrived(b):
        @pl.when(b != f)
        def _():
            bulk(facs.at[b, 0:half * part], s3.at[0], r3.at[b, 0]).wait_recv()
            bulk(infos.at[b, 0:half], s3.at[1], r3.at[b, 1]).wait_recv()

    def prepare(b, k):
        if k == 0:
            inf = jnp.concatenate([infos[b, p] for p in range(nc)], axis=1)
            bias, mu = inf[0:1], inf[1:2]
            caps[b] = inf
        else:
            g = (k - 1) * nf + b
            inf = caps[b]
            bias, cap = inf[0:1], inf[2:3]
            load = total_of(g)[:, 0:padded]
            mu = jnp.maximum(0.0, mus[g] + (0.1 / k) * (load - cap) / (load + jnp.where(cap > 0, cap, 1.0)))
        mus[k * nf + b] = mu
        parts = [p.astype(F32) for p in split3(bias) + split3(mu)]
        stack = jnp.concatenate([jnp.ones((3, padded), F32)] + parts + [jnp.zeros((7, padded), F32)], axis=0).astype(BF16)
        side[b] = lax.dot_general(stack, sel, (((0,), (0,)), ((), ())), preferred_element_type=F32).astype(BF16)

    def first_sum(g, e, peer):
        return pltpu.make_async_remote_copy(pay.at[g], got1.at[g, e], s4, r4.at[g], device_id=peer, device_id_type=MESH)

    def second_sum(g, d, peer):
        return pltpu.make_async_remote_copy(mid.at[g], got2.at[g, d], s5, r5.at[g], device_id=peer, device_id_type=MESH)

    def wait_second(g):
        bulk(got2.at[g], s5, r5.at[g]).wait_recv()

    def total_of(g):
        total = mid[g]
        for d in range(nf - 1):
            total = total + got2[g, d]
        return total

    def pass_on(g):
        bulk(got1.at[g], s4, r4.at[g]).wait_recv()
        total = pay[g]
        for e in range(nc - 1):
            total = total + got1[g, e]
        mid[g] = total
        for d in range(1, nf):
            second_sum(g, d - 1, (lax.rem(f + d, nf), c)).start()

    block = y_ref.shape[2]
    tiles = cols // block
    tall = y_ref.shape[1]
    groups = block // 128
    scale = math.log2(math.e) / 6.4

    def dot(b, t, slot):
        lhs = jnp.concatenate([facs[b, 0:tall], side[b, 0:tall]], axis=1)
        y_ref[slot] = jnp.dot(lhs, w_ref[:, t * block:(t + 1) * block], preferred_element_type=F32)

    def tile(b, t, slot):
        at = [slice(t * block + q * 128, t * block + (q + 1) * 128) for q in range(groups)]
        covs = [cov_ref[:, a] for a in at]
        softs = [soft_ref[:, a] for a in at]
        ds = [d_ref[:, a] for a in at]
        for r in range(0, rows, 32):
            size = min(4, (rows - r) // 8)
            sums = [None] * size
            for q in range(groups):
                us = [1.0 + jnp.exp2(y_ref[slot, r + 8 * s:r + 8 * s + 8, q * 128:(q + 1) * 128] * scale) for s in range(size)]
                gs = []
                p = None
                for s in range(0, size - 1, 2):
                    two = us[s] * us[s + 1]
                    inv = ds[q] * (1.0 / two)
                    gs += [us[s + 1] * inv, us[s] * inv]
                    p = two if p is None else p * two
                if size % 2:
                    gs.append(ds[q] * (1.0 / us[-1]))
                    p = us[-1] if p is None else p * us[-1]
                held = gs[0] if size == 1 else gs[0] + gs[1]
                if size == 3:
                    held = held + gs[2]
                if size == 4:
                    held = held + (gs[2] + gs[3])
                covs[q] = covs[q] + (float(size) * ds[q] - held)
                softs[q] = softs[q] + jnp.log2(p)
                sums = [g if v is None else v + g for v, g in zip(sums, gs)]
            for s in range(size):
                lo = r + 8 * s
                acc[b, lo:lo + 8, :] = sums[s] if t == 0 else acc[b, lo:lo + 8, :] + sums[s]
        for q in range(groups):
            cov_ref[:, at[q]] = covs[q]
            soft_ref[:, at[q]] = softs[q]

    ones16 = jnp.ones((16, 128), BF16)
    live = lax.broadcasted_iota(jnp.int32, (padded, 128), 0) < rows

    def row_of(b, g):
        part_sum = jnp.where(live, dl_ref[...] - acc[b], 0.0)
        hi = part_sum.astype(BF16)
        lo = (part_sum - hi.astype(F32)).astype(BF16)
        pay[g, :, 0:padded] = (nt(ones16, hi) + nt(ones16, lo))[0:1]

    def send_row(g):
        for e in range(nc - 1):
            first_sum(g, e, (f, lax.rem(c + e + 1, nc))).start()

    pair = f - lax.rem(f, 2)

    def place(k, p):
        if k > 0:
            return p
        q = p - 2
        far = q + 2 * ((q + nf - pair) // nf)
        return jnp.where(p == 0, f, jnp.where(p == 1, 2 * pair + 1 - f, far))

    def finish_step(k):
        wt = d_ref[0:1, :]
        lam = lam_ref[...]
        cover = jnp.sum(cov_ref[...], axis=0, keepdims=True) / wt
        soft = math.log(2.0) * jnp.sum(soft_ref[...], axis=0, keepdims=True)
        held = jnp.sum(mus[k * nf + f] * caps[f, 2:3])
        here = jnp.sum(wt * lam - TAU * wt * soft) - jnp.where(c == 0, held, 0.0)
        tot = tot_ref[...] + jnp.where(lane == k, here, 0.0)
        tot_ref[...] = tot
        lam = lam + (0.1 / (k + 1)) * wt * (1.0 - cover) / (1.0 + cover)
        lam_ref[...] = lam
        if k == ITERS - 1:
            pay[ITERS * nf - 1, :, wide - 128:] = tot
        else:
            set_aug(lam)

    def gather_turn(p):
        @pl.when(p == 0)
        def _():
            forward_first(place(0, 1))
            forward_side(place(0, 1))

            def each(i, _):
                forward_first(place(0, i))
                return 0

            lax.fori_loop(2, nf, each, 0)

        @pl.when((p > 0) & (2 * p < nf))
        def _():
            forward_side(place(0, 2 * p))
            forward_side(place(0, 2 * p + 1))

        @pl.when(p + 1 < nf)
        def _():
            arrived(place(0, p + 1))

    set_aug(lam)
    for k in range(ITERS):
        cov_ref[...] = jnp.zeros_like(cov_ref)
        soft_ref[...] = jnp.zeros_like(soft_ref)
        start = f if k == 0 else 0
        if k > 0:
            wait_second((k - 1) * nf)
        prepare(start, k)
        dot(start, 0, 0)

        def body(p, _, k=k):
            b = place(k, p)
            nxt = place(k, lax.rem(p + 1, nf))
            if k == 0:
                before = place(0, lax.rem(p + nf - 1, nf))
            elif k == 1:
                before = jnp.where(p == 0, place(0, nf - 1), nf + p - 1)
            else:
                before = k * nf + p - 1
            if k == 0:
                row_of(before, before)
            else:
                row_of(lax.rem(before, nf), before)
            for t in range(tiles // 2):
                dot(b, t + 1, (t + 1) % 2)
                tile(b, t, t % 2)
            if k == 0:
                @pl.when(p > 0)
                def _():
                    send_row(before)

                @pl.when(p >= LAG)
                def _():
                    pass_on(place(0, p - LAG))
                gather_turn(p)
            else:
                send_row(before)
                if k == 1:
                    pass_on(jnp.where(p < LAG, place(0, nf + p - LAG), nf + p - LAG))
                else:
                    pass_on(k * nf + p - LAG)

                @pl.when(p + 1 < nf)
                def _():
                    wait_second((k - 1) * nf + p + 1)
            for t in range(tiles // 2, tiles - 1):
                dot(b, t + 1, (t + 1) % 2)
                tile(b, t, t % 2)
            prepare(nxt, k)
            dot(nxt, 0, tiles % 2)
            tile(b, tiles - 1, (tiles - 1) % 2)
            return 0

        lax.fori_loop(0, nf, body, 0)
        finish_step(k)

    last = ITERS * nf
    row_of(nf - 1, last - 1)
    send_row(last - 1)

    for d in range(1, nf):
        pltpu.make_async_remote_copy(lam_ref, lam_out.at[f], s6, r6, device_id=(lax.rem(f + d, nf), c), device_id_type=MESH).start()
    lam_out[f] = lam_ref[...]

    @pl.when(core == 1)
    def _():
        bulk(facs.at[0:nf - 1, 0:2 * part], s1.at[0], r1.at[0, 0]).wait_send()
        bulk(infos.at[0:nf - 1, 0:2], s1.at[1], r1.at[0, 1]).wait_send()

    for send, recv, width_parts in ((s2, r2, half - 1), (s3, r3, half)):
        bulk(facs.at[0:nf - 1, 0:width_parts * part], send.at[0], recv.at[(0,) * (len(recv.shape) - 1) + (0,)]).wait_send()
        bulk(infos.at[0:nf - 1, 0:width_parts], send.at[1], recv.at[(0,) * (len(recv.shape) - 1) + (1,)]).wait_send()

    def flush(i, _):
        pass_on(last - LAG + i)
        return 0

    lax.fori_loop(0, LAG, flush, 0)

    def drain(i, _):
        wait_second(last - nf + i)
        return 0

    lax.fori_loop(0, nf, drain, 0)
    load = total_of(last - nf + f)[:, 0:padded]
    inf = caps[f]
    cap = inf[2:3]
    mu = mus[last - nf + f]
    mu = jnp.maximum(0.0, mu + (0.1 / ITERS) * (load - cap) / (load + jnp.where(cap > 0, cap, 1.0)))
    stack = jnp.concatenate([v.astype(F32) for v in split3(mu)] + [jnp.zeros((13, padded), F32)], axis=0).astype(BF16)
    back = jnp.dot(stack, hot_ref[...], preferred_element_type=F32)
    shut = mu_in_ref[...]
    for k in range(ITERS):
        shut = jnp.maximum(0.0, shut - 0.1 / (k + 1))
    cap_out[...] = jnp.where(open_ref[...] > 0, back[0:1] + back[1:2] + back[2:3], shut)
    bound_out[...] = total_of(last - 1)[:, wide - 128:] / total_cust
    if first:
        most = jnp.max(jnp.max(caps[:, 3, :], axis=0, keepdims=True), axis=1, keepdims=True)
        flag_out[0, 0] = (most[0, 0] > rows).astype(jnp.int32)

    lams = bulk(lam_out.at[0:nf - 1], s6, r6)
    lams.wait_send()
    lams.wait_recv()
    bulk(got1, s4, r4.at[0]).wait_send()
    bulk(got2, s5, r5.at[0]).wait_send()


def finish_kernel(lam_ref, cap_ref, bound_ref, lam_out, cap_out, bound_out):
    lam_out[...] = lam_ref[...]
    cap_out[...] = cap_ref[...]
    bound_out[...] = bound_ref[:, 0:bound_out.shape[1]]


def local(nf, nc, fac_coords, cust_coords, open_flags, demand, fixed_cost, capacity, cap_mult, cover_mult):
    n, width = fac_coords.shape
    cols = cust_coords.shape[0]
    sd = jax.ShapeDtypeStruct
    dma = pltpu.SemaphoreType.DMA
    half = nc // 2
    open_row = open_flags.reshape(1, n)
    block = math.gcd(cols, 256)
    small = (open_row, capacity.reshape(1, n), cap_mult.reshape(1, n), fixed_cost.reshape(1, n))
    large = (fac_coords, cust_coords, demand.reshape(1, nf * cols), cover_mult.reshape(1, nf * cols))

    def run(rows, cid, packed=None):
        part = -(-rows // (16 * nc)) * 16
        padded = part * nc
        wide = -(-padded // 128) * 128 + 128
        last = ITERS * nf
        first = packed is None
        return pl.pallas_call(
            functools.partial(solve_kernel, nf, nc, rows, cols * nf * nc, first),
            out_shape=(sd((nf, 1, cols), F32), sd((1, n), F32), sd((1, 128), F32)) + ((sd((1, 1), jnp.int32), sd((4, n), F32)) if first else ()),
            in_specs=[HBM] * 8 if first else [VMEM] + [HBM] * 4,
            out_specs=(VMEM,) * 3 + ((SMEM, VMEM) if first else ()),
            scratch_shapes=[
                pltpu.VMEM((1, n), jnp.int32),
                pltpu.VMEM((n, width), BF16),
                pltpu.VMEM((1, n), F32),
                pltpu.VMEM((1, n), F32),
                pltpu.VMEM((1, n), F32),
                pltpu.VMEM((cols, width), BF16),
                pltpu.VMEM((1, cols), jnp.int32),
                pltpu.VMEM((1, cols), F32),
                dma((8,)),
                pltpu.VMEM((nf, padded, width), BF16),
                pltpu.VMEM((nf, nc, 4, part), F32),
                pltpu.VMEM((padded, n), BF16),
                pltpu.VMEM((nf, padded, width), BF16),
                pltpu.VMEM((2 * width, cols), BF16),
                pltpu.VMEM((2, -(-rows // 16) * 16, block), F32),
                pltpu.VMEM((nf, padded, 128), F32),
                pltpu.VMEM((8, cols), F32),
                pltpu.VMEM((8, cols), F32),
                pltpu.VMEM((8, cols), F32),
                pltpu.VMEM((1, cols), F32),
                pltpu.VMEM((1, cols), F32),
                pltpu.VMEM((last, 1, padded), F32),
                pltpu.VMEM((nf, 4, padded), F32),
                pltpu.VMEM((1, 128), F32),
                pltpu.VMEM((1, 128), F32),
                pltpu.VMEM((last, 1, wide), F32),
                pltpu.VMEM((last, nc - 1, 1, wide), F32),
                pltpu.VMEM((last, 1, wide), F32),
                pltpu.VMEM((last, nf - 1, 1, wide), F32),
                dma((2,)), dma((nf, 2)),
                dma((2,)), dma((nf, half - 1, 2)),
                dma((2,)), dma((nf, 2)),
                dma(()), dma((last,)), dma(()), dma((last,)),
                dma(()), dma(()),
            ],
            compiler_params=pltpu.CompilerParams(collective_id=cid, has_side_effects=True, vmem_limit_bytes=56 * 2 ** 20),
            name="solve",
        )(*(small if first else (packed,)), *large)

    rows = min(n, -(-int(n / 2 + 1.75 * math.sqrt(n)) // 8) * 8)
    lam, cap, bound, flag, packed = run(rows, 0)
    if rows < n:
        lam, cap, bound = lax.cond(flag[0, 0] > 0, lambda: tuple(run(n, 1, packed)), lambda: (lam, cap, bound))
    lam, cap, bound = pl.pallas_call(
        finish_kernel, out_shape=(sd((nf, 1, cols), F32), sd((1, n), F32), sd((1, ITERS), F32)),
        in_specs=[VMEM] * 3, out_specs=(VMEM,) * 3, name="finish",
    )(lam, cap, bound)
    return lam.reshape(nf * cols), cap.reshape(n), bound.reshape(ITERS)


def solution(mesh):
    nf, nc = mesh.shape["fac"], mesh.shape["cust"]
    return jax.shard_map(
        functools.partial(local, nf, nc),
        mesh=mesh,
        in_specs=(P("fac", None), P(("cust", "fac"), None), P("fac"), P("cust"), P("fac"), P("fac"), P("fac"), P("cust")),
        out_specs=(P("cust"), P("fac"), P()),
        check_vma=False,
    )
```

```python
import functools
import math

import jax
import jax.numpy as jnp
from jax import lax
from jax.experimental import pallas as pl
from jax.experimental.pallas import tpu as pltpu
from jax.sharding import PartitionSpec as P

MESH = pl.DeviceIdType.MESH
ITERS = 3
TAU = 0.1
LAG = 3
CLOSED = -30000.0
F32 = jnp.float32
BF16 = jnp.bfloat16
VMEM = pl.BlockSpec(memory_space=pltpu.VMEM)
SMEM = pl.BlockSpec(memory_space=pltpu.SMEM)
HBM = pl.BlockSpec(memory_space=pltpu.HBM)


def split3(v):
    a = v.astype(BF16)
    r = v - a.astype(F32)
    b = r.astype(BF16)
    c = (r - b.astype(F32)).astype(BF16)
    return a, b, c


def nt(a, b):
    return lax.dot_general(a, b, (((1,), (1,)), ((), ())), preferred_element_type=F32)


def eye_of(rows, width):
    hit = lax.broadcasted_iota(jnp.int32, (rows, width), 0) == lax.broadcasted_iota(jnp.int32, (rows, width), 1)
    return hit.astype(F32).astype(BF16)


def onehot_of(open_row, rows):
    n = open_row.shape[1]
    flags = jnp.broadcast_to(open_row.astype(F32), (16, n)).astype(BF16)
    tri = (lax.broadcasted_iota(jnp.int32, (n, n), 0) <= lax.broadcasted_iota(jnp.int32, (n, n), 1)).astype(F32).astype(BF16)
    pos = jnp.dot(flags, tri, preferred_element_type=F32)[0:1]
    pos = jnp.where(open_row > 0, pos - 1.0, -1.0).astype(jnp.int32)
    hit = lax.broadcasted_iota(jnp.int32, (rows, n), 0) == pos
    return jnp.where(hit, 1.0, 0.0).astype(BF16)


def solve_kernel(nf, nc, rows, total_cust,
                 first, *refs):
    small_in, (fac_in, cust_in, demand_in, cover_in), refs = (refs[:4], refs[4:8], refs[8:]) if first else (refs[0], refs[1:5], refs[5:])
    (lam_out, cap_out, bound_out), refs = refs[:3], refs[3:]
    if first:
        (flag_out, small_out), refs = refs[:2], refs[2:]
    (open_ref, fac_ref, cap_ref, mu_in_ref, fixed_ref, cust_ref, demand_ref, cover_ref, loads,
                 facs, infos, hot_ref, side, w_ref, y_ref, acc, cov_ref, soft_ref, d_ref, hq_ref, lam_ref, mus, caps,
                 tot_ref, dl_ref, pay, got1, mid, got2,
                 s1, r1, s2, r2, s3, r3, s4, r4, s5, r5, s6, r6) = refs
    f, c = lax.axis_index("fac"), lax.axis_index("cust")
    n, width = fac_ref.shape
    cols = cust_ref.shape[0]
    part = infos.shape[3]
    padded = part * nc
    wide = pay.shape[2]
    half = nc // 2
    core = lax.rem(c, 2)
    twin = (f, c + 1 - 2 * core)
    barrier = pltpu.get_barrier_semaphore()
    for d in range(1, nf):
        pl.semaphore_signal(barrier, inc=1, device_id=(lax.rem(f + d, nf), c), device_id_type=MESH)
        pl.semaphore_signal(barrier, inc=1, device_id=(lax.rem(f + d, nf), twin[1]), device_id_type=MESH)
    for d in range(1, nc):
        pl.semaphore_signal(barrier, inc=1, device_id=(f, lax.rem(c + d, nc)), device_id_type=MESH)

    mine = pl.ds(pl.multiple_of(f * cols, cols), cols)
    pairs = [(fac_in, fac_ref), (cust_in, cust_ref), (demand_in.at[:, mine], demand_ref), (cover_in.at[:, mine], cover_ref)]
    if first:
        pairs += list(zip(small_in, (open_ref, cap_ref, mu_in_ref, fixed_ref)))
    fetch = [pltpu.make_async_copy(src, dst, loads.at[i]) for i, (src, dst) in enumerate(pairs)]
    for cpy in fetch:
        cpy.start()
    for cpy in fetch[:1] + fetch[4:]:
        cpy.wait()
    if first:
        small_out[0:1, :] = open_ref[...].astype(F32)
        for i, ref in enumerate((cap_ref, mu_in_ref, fixed_ref)):
            small_out[i + 1:i + 2, :] = ref[...]
    else:
        open_ref[...] = small_in[0:1, :].astype(jnp.int32)
        for i, ref in enumerate((cap_ref, mu_in_ref, fixed_ref)):
            ref[...] = small_in[i + 1:i + 2, :]

    opened = open_ref[...].astype(F32)
    hot = onehot_of(open_ref[...], padded)
    hot_ref[...] = hot
    fac = fac_ref[...]
    facs[f] = jnp.dot(hot, fac, preferred_element_type=F32).astype(BF16)
    q1, q2, _ = split3(fac.astype(F32) ** 2)
    ones = jnp.ones((16, width), BF16)
    halfsq = -0.5 * (nt(ones, q1) + nt(ones, q2))[0:1]
    rows16 = [jnp.ones((1, n), BF16)]
    for v in (halfsq, mu_in_ref[...], cap_ref[...]):
        rows16.extend(split3(v))
    rows16 = [r.astype(F32) for r in rows16] + [jnp.zeros((6, n), F32)]
    got = nt(jnp.concatenate(rows16, axis=0).astype(BF16), hot)
    bias = jnp.where(got[0:1] > 0, got[1:2] + got[2:3] + got[3:4], CLOSED)
    count = jnp.broadcast_to(jnp.sum(opened, axis=1, keepdims=True), (1, padded))
    info = jnp.concatenate([bias, got[4:5] + got[5:6] + got[6:7], got[7:8] + got[8:9] + got[9:10], count], axis=0)
    for p in range(nc):
        infos[f, p] = info[:, p * part:(p + 1) * part]

    def rows_of(q):
        return pl.ds(pl.multiple_of(q * part, 16), part)

    def bulk(ref, send, recv):
        return pltpu.make_async_remote_copy(ref, ref, send, recv, device_id=twin, device_id_type=MESH)

    def move(src, q, send, recv, peer):
        a, b = facs.at[src, rows_of(q)], infos.at[src, q]
        return [pltpu.make_async_remote_copy(a, a, send.at[0], recv.at[0], device_id=peer, device_id_type=MESH),
                pltpu.make_async_remote_copy(b, b, send.at[1], recv.at[1], device_id=peer, device_id_type=MESH)]

    def first_copy(src, peer_f, peer_c):
        return move(src, peer_c, s1, r1.at[src], (peer_f, peer_c))

    def side_copy(src, e, q):
        return move(src, q, s2, r2.at[src, e], (f, lax.rem(c + 2 * (e + 1), nc)))

    def twin_copy(src, q):
        return move(src, q, s3, r3.at[src], twin)

    pl.semaphore_wait(barrier, 2 * (nf - 1) + nc - 1)
    upper = f // (nf // 2)

    @pl.when(core == 1)
    def _():
        for j in range(nf - 1):
            down = nf - 2 - j + (nf - 2 - j + nf - f) // nf
            up = j + (j + nf - f) // nf
            for peer_c in (c - 1, c):
                for cpy in first_copy(f, upper * up + (1 - upper) * down, peer_c):
                    cpy.start()

    for cpy in fetch[1:4]:
        cpy.wait()
    ext = jnp.zeros((1, 128), F32)
    lane = lax.broadcasted_iota(jnp.int32, (1, 128), 1)
    shut = mu_in_ref[...]
    for k in range(ITERS):
        fixed = jnp.sum(opened * fixed_ref[...] - (1.0 - opened) * shut * cap_ref[...])
        ext = ext + jnp.where((lane == k) & (c == 0), fixed, 0.0)
        shut = jnp.maximum(0.0, shut - 0.1 / (k + 1))
    tot_ref[...] = ext
    wt = demand_ref[...].astype(F32)
    lam = cover_ref[...]
    lam_ref[...] = lam
    d_ref[...] = jnp.broadcast_to(wt, (8, cols))
    turned = nt(eye_of(width, width), cust_ref[...])
    w_ref[0:width, :] = turned.astype(BF16)
    hq = 0.5 * jnp.sum(turned * turned, axis=0, keepdims=True)
    hq_ref[...] = hq
    w_ref[width:, :] = jnp.zeros((width, cols), BF16)
    sel = eye_of(16, width)
    acc[...] = jnp.zeros_like(acc)
    lanes_d = jnp.zeros((1, 128), F32)
    for t in range(cols // 128):
        lanes_d = lanes_d + wt[:, t * 128:(t + 1) * 128]
    dl_ref[...] = lanes_d
    pay[...] = jnp.zeros_like(pay)

    def set_aug(lam):
        a1, a2, a3 = split3(64.0 * lam - hq_ref[...])
        aug = jnp.concatenate([a1.astype(F32), a2.astype(F32), a3.astype(F32), jnp.ones((3, cols), F32),
                               jnp.broadcast_to(-64.0 * d_ref[0:1, :], (3, cols)), jnp.zeros((7, cols), F32)], axis=0)
        w_ref[width:width + 16, :] = aug.astype(BF16)

    def forward_first(b):
        @pl.when(b != f)
        def _():
            for cpy in first_copy(b, f, c):
                cpy.wait_recv()
            for e in range(half - 1):
                for cpy in side_copy(b, e, c):
                    cpy.start()
            for cpy in twin_copy(b, c):
                cpy.start()

    def forward_side(b):
        @pl.when(b != f)
        def _():
            for e in range(half - 1):
                q = lax.rem(c + nc - 2 * (e + 1), nc)
                for cpy in side_copy(b, e, q):
                    cpy.wait_recv()
                for cpy in twin_copy(b, q):
                    cpy.start()

    def arrived(b):
        @pl.when(b != f)
        def _():
            bulk(facs.at[b, 0:half * part], s3.at[0], r3.at[b, 0]).wait_recv()
            bulk(infos.at[b, 0:half], s3.at[1], r3.at[b, 1]).wait_recv()

    def prepare(b, k):
        if k == 0:
            inf = jnp.concatenate([infos[b, p] for p in range(nc)], axis=1)
            bias, mu = inf[0:1], inf[1:2]
            caps[b] = inf
        else:
            g = (k - 1) * nf + b
            inf = caps[b]
            bias, cap = inf[0:1], inf[2:3]
            load = total_of(g)[:, 0:padded]
            mu = jnp.maximum(0.0, mus[g] + (0.1 / k) * (load - cap) / (load + jnp.where(cap > 0, cap, 1.0)))
        mus[k * nf + b] = mu
        parts = [p.astype(F32) for p in split3(bias) + split3(mu)]
        stack = jnp.concatenate([jnp.ones((3, padded), F32)] + parts + [jnp.zeros((7, padded), F32)], axis=0).astype(BF16)
        side[b] = lax.dot_general(stack, sel, (((0,), (0,)), ((), ())), preferred_element_type=F32).astype(BF16)

    def first_sum(g, e, peer):
        return pltpu.make_async_remote_copy(pay.at[g], got1.at[g, e], s4, r4.at[g], device_id=peer, device_id_type=MESH)

    def second_sum(g, d, peer):
        return pltpu.make_async_remote_copy(mid.at[g], got2.at[g, d], s5, r5.at[g], device_id=peer, device_id_type=MESH)

    def wait_second(g):
        bulk(got2.at[g], s5, r5.at[g]).wait_recv()

    def total_of(g):
        total = mid[g]
        for d in range(nf - 1):
            total = total + got2[g, d]
        return total

    def pass_on(g):
        bulk(got1.at[g], s4, r4.at[g]).wait_recv()
        total = pay[g]
        for e in range(nc - 1):
            total = total + got1[g, e]
        mid[g] = total
        for d in range(1, nf):
            second_sum(g, d - 1, (lax.rem(f + d, nf), c)).start()

    block = y_ref.shape[2]
    tiles = cols // block
    tall = y_ref.shape[1]
    groups = block // 128
    scale = math.log2(math.e) / 6.4

    def dot(b, t, slot):
        lhs = jnp.concatenate([facs[b, 0:tall], side[b, 0:tall]], axis=1)
        y_ref[slot] = jnp.dot(lhs, w_ref[:, t * block:(t + 1) * block], preferred_element_type=F32)

    def tile(b, t, slot):
        at = [slice(t * block + q * 128, t * block + (q + 1) * 128) for q in range(groups)]
        covs = [cov_ref[:, a] for a in at]
        softs = [soft_ref[:, a] for a in at]
        ds = [d_ref[:, a] for a in at]
        for r in range(0, rows, 32):
            size = min(4, (rows - r) // 8)
            sums = [None] * size
            for q in range(groups):
                es = [jnp.exp2(y_ref[slot, r + 8 * s:r + 8 * s + 8, q * 128:(q + 1) * 128] * scale) for s in range(size)]
                xs = []
                p = None
                for s in range(0, size - 1, 2):
                    both = es[s] * es[s + 1]
                    left, right = es[s] + both, es[s + 1] + both
                    two = (1.0 + es[s]) + right
                    inv = ds[q] * (1.0 / two)
                    xs += [left * inv, right * inv]
                    p = two if p is None else p * two
                if size % 2:
                    one = 1.0 + es[-1]
                    xs.append(es[-1] * (ds[q] * (1.0 / one)))
                    p = one if p is None else p * one
                total = xs[0] if size == 1 else xs[0] + xs[1]
                if size == 3:
                    total = total + xs[2]
                if size == 4:
                    total = total + (xs[2] + xs[3])
                covs[q] = covs[q] + total
                softs[q] = softs[q] + jnp.log2(p)
                sums = [x if v is None else v + x for v, x in zip(sums, xs)]
            for s in range(size):
                lo = r + 8 * s
                acc[b, lo:lo + 8, :] = sums[s] if t == 0 else acc[b, lo:lo + 8, :] + sums[s]
        for q in range(groups):
            cov_ref[:, at[q]] = covs[q]
            soft_ref[:, at[q]] = softs[q]

    ones16 = jnp.ones((16, 128), BF16)

    def row_of(b, g):
        part_sum = acc[b]
        hi = part_sum.astype(BF16)
        lo = (part_sum - hi.astype(F32)).astype(BF16)
        pay[g, :, 0:padded] = (nt(ones16, hi) + nt(ones16, lo))[0:1]

    def send_row(g):
        for e in range(nc - 1):
            first_sum(g, e, (f, lax.rem(c + e + 1, nc))).start()

    pair = f - lax.rem(f, 2)

    def place(k, p):
        if k > 0:
            return p
        q = p - 2
        far = q + 2 * ((q + nf - pair) // nf)
        return jnp.where(p == 0, f, jnp.where(p == 1, 2 * pair + 1 - f, far))

    def finish_step(k):
        wt = d_ref[0:1, :]
        lam = lam_ref[...]
        cover = jnp.sum(cov_ref[...], axis=0, keepdims=True) / wt
        soft = math.log(2.0) * jnp.sum(soft_ref[...], axis=0, keepdims=True)
        held = jnp.sum(mus[k * nf + f] * caps[f, 2:3])
        here = jnp.sum(wt * lam - TAU * wt * soft) - jnp.where(c == 0, held, 0.0)
        tot = tot_ref[...] + jnp.where(lane == k, here, 0.0)
        tot_ref[...] = tot
        lam = lam + (0.1 / (k + 1)) * wt * (1.0 - cover) / (1.0 + cover)
        lam_ref[...] = lam
        if k == ITERS - 1:
            pay[ITERS * nf - 1, :, wide - 128:] = tot
        else:
            set_aug(lam)

    def gather_turn(p):
        @pl.when(p == 0)
        def _():
            forward_first(place(0, 1))
            forward_side(place(0, 1))

            def each(i, _):
                forward_first(place(0, i))
                return 0

            lax.fori_loop(2, nf, each, 0)

        @pl.when((p > 0) & (2 * p < nf))
        def _():
            forward_side(place(0, 2 * p))
            forward_side(place(0, 2 * p + 1))

        @pl.when(p + 1 < nf)
        def _():
            arrived(place(0, p + 1))

    set_aug(lam)
    for k in range(ITERS):
        cov_ref[...] = jnp.zeros_like(cov_ref)
        soft_ref[...] = jnp.zeros_like(soft_ref)
        start = f if k == 0 else 0
        if k > 0:
            wait_second((k - 1) * nf)
        prepare(start, k)
        dot(start, 0, 0)

        def body(p, _, k=k):
            b = place(k, p)
            nxt = place(k, lax.rem(p + 1, nf))
            if k == 0:
                before = place(0, lax.rem(p + nf - 1, nf))
            elif k == 1:
                before = jnp.where(p == 0, place(0, nf - 1), nf + p - 1)
            else:
                before = k * nf + p - 1
            if k == 0:
                row_of(before, before)
            else:
                row_of(lax.rem(before, nf), before)
            for t in range(tiles // 2):
                dot(b, t + 1, (t + 1) % 2)
                tile(b, t, t % 2)
            if k == 0:
                @pl.when(p > 0)
                def _():
                    send_row(before)

                @pl.when(p >= LAG)
                def _():
                    pass_on(place(0, p - LAG))
                gather_turn(p)
            else:
                send_row(before)
                if k == 1:
                    pass_on(jnp.where(p < LAG, place(0, nf + p - LAG), nf + p - LAG))
                else:
                    pass_on(k * nf + p - LAG)

                @pl.when(p + 1 < nf)
                def _():
                    wait_second((k - 1) * nf + p + 1)
            for t in range(tiles // 2, tiles - 1):
                dot(b, t + 1, (t + 1) % 2)
                tile(b, t, t % 2)
            prepare(nxt, k)
            dot(nxt, 0, tiles % 2)
            tile(b, tiles - 1, (tiles - 1) % 2)
            return 0

        lax.fori_loop(0, nf, body, 0)
        finish_step(k)

    last = ITERS * nf
    row_of(nf - 1, last - 1)
    send_row(last - 1)

    for d in range(1, nf):
        pltpu.make_async_remote_copy(lam_ref, lam_out.at[f], s6, r6, device_id=(lax.rem(f + d, nf), c), device_id_type=MESH).start()
    lam_out[f] = lam_ref[...]

    @pl.when(core == 1)
    def _():
        bulk(facs.at[0:nf - 1, 0:2 * part], s1.at[0], r1.at[0, 0]).wait_send()
        bulk(infos.at[0:nf - 1, 0:2], s1.at[1], r1.at[0, 1]).wait_send()

    for send, recv, width_parts in ((s2, r2, half - 1), (s3, r3, half)):
        bulk(facs.at[0:nf - 1, 0:width_parts * part], send.at[0], recv.at[(0,) * (len(recv.shape) - 1) + (0,)]).wait_send()
        bulk(infos.at[0:nf - 1, 0:width_parts], send.at[1], recv.at[(0,) * (len(recv.shape) - 1) + (1,)]).wait_send()

    def flush(i, _):
        pass_on(last - LAG + i)
        return 0

    lax.fori_loop(0, LAG, flush, 0)

    def drain(i, _):
        wait_second(last - nf + i)
        return 0

    lax.fori_loop(0, nf, drain, 0)
    load = total_of(last - nf + f)[:, 0:padded]
    inf = caps[f]
    cap = inf[2:3]
    mu = mus[last - nf + f]
    mu = jnp.maximum(0.0, mu + (0.1 / ITERS) * (load - cap) / (load + jnp.where(cap > 0, cap, 1.0)))
    stack = jnp.concatenate([v.astype(F32) for v in split3(mu)] + [jnp.zeros((13, padded), F32)], axis=0).astype(BF16)
    back = jnp.dot(stack, hot_ref[...], preferred_element_type=F32)
    shut = mu_in_ref[...]
    for k in range(ITERS):
        shut = jnp.maximum(0.0, shut - 0.1 / (k + 1))
    cap_out[...] = jnp.where(open_ref[...] > 0, back[0:1] + back[1:2] + back[2:3], shut)
    bound_out[...] = total_of(last - 1)[:, wide - 128:] / total_cust
    if first:
        most = jnp.max(jnp.max(caps[:, 3, :], axis=0, keepdims=True), axis=1, keepdims=True)
        flag_out[0, 0] = (most[0, 0] > rows).astype(jnp.int32)

    lams = bulk(lam_out.at[0:nf - 1], s6, r6)
    lams.wait_send()
    lams.wait_recv()
    bulk(got1, s4, r4.at[0]).wait_send()
    bulk(got2, s5, r5.at[0]).wait_send()


def finish_kernel(lam_ref, cap_ref, bound_ref, lam_out, cap_out, bound_out):
    lam_out[...] = lam_ref[...]
    cap_out[...] = cap_ref[...]
    bound_out[...] = bound_ref[:, 0:bound_out.shape[1]]


def local(nf, nc, fac_coords, cust_coords, open_flags, demand, fixed_cost, capacity, cap_mult, cover_mult):
    n, width = fac_coords.shape
    cols = cust_coords.shape[0]
    sd = jax.ShapeDtypeStruct
    dma = pltpu.SemaphoreType.DMA
    half = nc // 2
    open_row = open_flags.reshape(1, n)
    block = math.gcd(cols, 256)
    small = (open_row, capacity.reshape(1, n), cap_mult.reshape(1, n), fixed_cost.reshape(1, n))
    large = (fac_coords, cust_coords, demand.reshape(1, nf * cols), cover_mult.reshape(1, nf * cols))

    def run(rows, cid, packed=None):
        part = -(-rows // (16 * nc)) * 16
        padded = part * nc
        wide = -(-padded // 128) * 128 + 128
        last = ITERS * nf
        first = packed is None
        return pl.pallas_call(
            functools.partial(solve_kernel, nf, nc, rows, cols * nf * nc, first),
            out_shape=(sd((nf, 1, cols), F32), sd((1, n), F32), sd((1, 128), F32)) + ((sd((1, 1), jnp.int32), sd((4, n), F32)) if first else ()),
            in_specs=[HBM] * 8 if first else [VMEM] + [HBM] * 4,
            out_specs=(VMEM,) * 3 + ((SMEM, VMEM) if first else ()),
            scratch_shapes=[
                pltpu.VMEM((1, n), jnp.int32),
                pltpu.VMEM((n, width), BF16),
                pltpu.VMEM((1, n), F32),
                pltpu.VMEM((1, n), F32),
                pltpu.VMEM((1, n), F32),
                pltpu.VMEM((cols, width), BF16),
                pltpu.VMEM((1, cols), jnp.int32),
                pltpu.VMEM((1, cols), F32),
                dma((8,)),
                pltpu.VMEM((nf, padded, width), BF16),
                pltpu.VMEM((nf, nc, 4, part), F32),
                pltpu.VMEM((padded, n), BF16),
                pltpu.VMEM((nf, padded, width), BF16),
                pltpu.VMEM((2 * width, cols), BF16),
                pltpu.VMEM((2, -(-rows // 16) * 16, block), F32),
                pltpu.VMEM((nf, padded, 128), F32),
                pltpu.VMEM((8, cols), F32),
                pltpu.VMEM((8, cols), F32),
                pltpu.VMEM((8, cols), F32),
                pltpu.VMEM((1, cols), F32),
                pltpu.VMEM((1, cols), F32),
                pltpu.VMEM((last, 1, padded), F32),
                pltpu.VMEM((nf, 4, padded), F32),
                pltpu.VMEM((1, 128), F32),
                pltpu.VMEM((1, 128), F32),
                pltpu.VMEM((last, 1, wide), F32),
                pltpu.VMEM((last, nc - 1, 1, wide), F32),
                pltpu.VMEM((last, 1, wide), F32),
                pltpu.VMEM((last, nf - 1, 1, wide), F32),
                dma((2,)), dma((nf, 2)),
                dma((2,)), dma((nf, half - 1, 2)),
                dma((2,)), dma((nf, 2)),
                dma(()), dma((last,)), dma(()), dma((last,)),
                dma(()), dma(()),
            ],
            compiler_params=pltpu.CompilerParams(collective_id=cid, has_side_effects=True, vmem_limit_bytes=56 * 2 ** 20),
            name="solve",
        )(*(small if first else (packed,)), *large)

    rows = min(n, -(-int(n / 2 + 1.75 * math.sqrt(n)) // 8) * 8)
    lam, cap, bound, flag, packed = run(rows, 0)
    if rows < n:
        lam, cap, bound = lax.cond(flag[0, 0] > 0, lambda: tuple(run(n, 1, packed)), lambda: (lam, cap, bound))
    lam, cap, bound = pl.pallas_call(
        finish_kernel, out_shape=(sd((nf, 1, cols), F32), sd((1, n), F32), sd((1, ITERS), F32)),
        in_specs=[VMEM] * 3, out_specs=(VMEM,) * 3, name="finish",
    )(lam, cap, bound)
    return lam.reshape(nf * cols), cap.reshape(n), bound.reshape(ITERS)


def solution(mesh):
    nf, nc = mesh.shape["fac"], mesh.shape["cust"]
    return jax.shard_map(
        functools.partial(local, nf, nc),
        mesh=mesh,
        in_specs=(P("fac", None), P(("cust", "fac"), None), P("fac"), P("cust"), P("fac"), P("fac"), P("fac"), P("cust")),
        out_specs=(P("cust"), P("fac"), P()),
        check_vma=False,
    )
```
